32 devices in a mesh: group: 2 (over x), seq: 16 (over z, y, core).
Axes of the slice: x: 2, y: 2, z: 4, core: 2. Of those that a mesh axis runs over, the one named last changes fastest.
Arguments:
- tokens: bfloat16 [16384, 2048], P(('group', 'seq')), parts along dimension 0, may hold values from -6 to 6
- w_qkv: bfloat16 [2048, 3072], P('seq'), may hold values from -0.125 to 0.125
- w_out: bfloat16 [1024, 2048], P('seq'), may hold values from -0.1875 to 0.1875
- level_weight: float32 [14, 4, 16384], P(None, None, ('group', 'seq')), parts along dimension 2, may hold values from 0.1 to 1
Outputs:
- mixed: bfloat16 [16384, 2048], P(('group', 'seq')), parts along dimension 0
The draws below stay inside these ranges and needn't reach their ends.
There are 2 independent parts, one for each index of `group`. The reference program is written for one: setup_inputs(seed, part) draws one part's arguments, and reference() takes and returns one part's arrays. A program takes and returns all parts, laid end to end along the dimension named above; an argument that names none is the same for every part. Nothing has to cross between parts.
All inputs are finite; a program needn't handle non-finite values.
Results may differ from the reference program's by a relative error of at most 0.0085.
Values may be sent and summed in bfloat16 or wider, within the bound.
No kernel may reach another device: no remote copies, remote signals or barrier semaphores. Data moves between devices by JAX's collectives and lax.ppermute only.
A program may use at most 128 MiB of HBM per device.

```python
import math
import jax
import jax.numpy as jnp
from jax import lax

D = 2048
HEADS = 4
HEAD = 256
SPAN = 256
TOKENS = 8192
NCHUNK = 32
CBITS = 8
NBITS = 5
LEVELS = 14


def level_of(stream_key, shape, split, smallest, top_value):
    factor_of, own = 1.0, jax.random.fold_in(stream_key, 6)
    for axis_at, parts in split:
        draws = jnp.exp(jax.random.uniform(jax.random.fold_in(own, axis_at), (parts,), jnp.float32, smallest / len(split), top_value / len(split)))
        factor_of = factor_of * jnp.repeat(draws, shape[axis_at] // parts).reshape([-1 if axis == axis_at else 1 for axis in range(len(shape))])
    return factor_of


def bell_draw(stream_key, shape, width, limit, split=(), held_as=jnp.bfloat16):
    factor_of = level_of(stream_key, shape, split, -0.22, 0.18) if split else 1.0
    entries = jax.random.normal(stream_key, shape, jnp.float32) * width * factor_of
    return jnp.minimum(jnp.maximum(entries, -limit), limit).astype(held_as)


def setup_inputs(seed: int = 0, part: int = 0) -> dict:
    seeds = jax.random.split(jax.random.key(seed), 5)
    own_keys = jax.random.split(jax.random.fold_in(seeds[4], part), 5)
    return {
        "tokens": bell_draw(own_keys[0], (TOKENS, D), 1.0, 6.0, ((0, 16),)),
        "w_qkv": bell_draw(seeds[1], (D, 3 * HEADS * HEAD), D ** -0.5, 0.125, ((0, 16),)),
        "w_out": bell_draw(seeds[2], (HEADS * HEAD, D), (HEADS * HEAD) ** -0.5, 0.1875, ((0, 16),)),
        "level_weight": jnp.clip(jnp.exp(math.log(1.0) - 2.3025851 * jax.random.uniform(own_keys[3], (LEVELS, HEADS, TOKENS), jnp.float32) ** level_of(own_keys[3], (LEVELS, HEADS, TOKENS), ((2, 16),), -0.2, 0.2)), 0.1, 1.0),
    }


def bit_length_of(values):
    result = jnp.zeros(values.shape, jnp.int32)
    for bit_pos in range(24):
        result = result + (values >= 1 << bit_pos).astype(jnp.int32)
    return result

def intra_table(span, cbits, head):
    position = jnp.arange(span, dtype=jnp.int32)
    pair_level = bit_length_of(position[:, None] ^ position[None, :])
    causal = position[:, None] >= position[None, :]
    levels_all = jnp.arange(cbits + 1, dtype=jnp.int32)
    gains = jnp.asarray([1.0 / math.sqrt(head * max(1, 2 ** (level_no - 1))) for level_no in range(cbits + 1)], jnp.float32)
    onehot = ((pair_level[None] == levels_all[:, None, None]) & causal[None]).astype(jnp.float32)
    return onehot * gains[:, None, None]

def reference(tokens, w_qkv, w_out, level_weight):
    highest = lax.Precision.HIGHEST
    head_cols = HEADS * HEAD
    qkv = jnp.dot(tokens, w_qkv, preferred_element_type=jnp.float32).astype(jnp.bfloat16)
    queries = qkv[:, :head_cols].reshape(NCHUNK, SPAN, HEADS, HEAD).astype(jnp.float32)
    key_rows = qkv[:, head_cols:2 * head_cols].reshape(NCHUNK, SPAN, HEADS, HEAD).astype(jnp.float32)
    value_rows = qkv[:, 2 * head_cols:].reshape(NCHUNK, SPAN, HEADS, HEAD).astype(jnp.float32)
    weights = level_weight.reshape(LEVELS, HEADS, NCHUNK, SPAN)
    table = intra_table(SPAN, CBITS, HEAD)
    mixing = jnp.einsum('lij,lhci->chij', table, weights[:CBITS + 1], precision=highest)
    scores = jnp.einsum('cihe,cjhe->chij', queries, key_rows, precision=highest)
    probs = (scores * mixing).astype(jnp.bfloat16)
    probs = lax.optimization_barrier(probs).astype(jnp.float32)
    intra = jnp.einsum('chij,cjhe->cihe', probs, value_rows, precision=highest)
    states = jnp.einsum('cjhe,cjhf->chef', key_rows, value_rows, precision=highest)
    inter = jnp.zeros((NCHUNK, SPAN, HEADS, HEAD), jnp.float32)
    for level_no in range(1, NBITS + 1):
        half_size = 2 ** (level_no - 1)
        blocks = NCHUNK // (2 * half_size)
        left = states.reshape(blocks, 2, half_size, HEADS, HEAD, HEAD)[:, 0].sum(axis=1)
        right_q = queries.reshape(blocks, 2, half_size, SPAN, HEADS, HEAD)[:, 1]
        read = jnp.einsum('bmihe,bhef->bmihf', right_q, left, precision=highest)
        scale = weights[CBITS + level_no].reshape(HEADS, blocks, 2, half_size, SPAN)[:, :, 1]
        scale = jnp.transpose(scale, (1, 2, 3, 0)) * (1.0 / math.sqrt(SPAN * half_size * HEAD))
        shaped = inter.reshape(blocks, 2, half_size, SPAN, HEADS, HEAD)
        inter = shaped.at[:, 1].add(read * scale[..., None]).reshape(NCHUNK, SPAN, HEADS, HEAD)
    attended = (intra + inter).reshape(TOKENS, head_cols).astype(jnp.bfloat16)
    return jnp.dot(attended, w_out, preferred_element_type=jnp.float32).astype(jnp.bfloat16)
```

```python
import functools
import math

import jax
import jax.numpy as jnp
from jax import lax
from jax.experimental import pallas as pl
from jax.experimental.pallas import tpu as pltpu
from jax.sharding import PartitionSpec as P

HEADS = 4
HEAD = 256
SPAN = 256
CBITS = 8
CORES = 2
F32 = jnp.float32
BF16 = jnp.bfloat16


def swap(value, bit):
    mask = 1 << bit
    return lax.ppermute(value, "seq", [(i, i ^ mask) for i in range(lax.axis_size("seq"))])


def swap_x(value):
    return lax.ppermute(value, "group", [(i, i ^ 1) for i in range(lax.axis_size("group"))])


def stacked(parts):
    return parts[0] if len(parts) == 1 else jnp.concatenate(parts, axis=0)


def gather_rows(own, other, zbits, groups_first):
    rows = own.shape[0]
    pieces, table = [], []

    def note(piece, entries):
        pieces.append(piece)
        for at, (flip, is_other) in enumerate(entries):
            table.append((len(pieces) - 1, at * rows, flip, is_other))

    parts, held = [(own, [0])], [own]
    for order, bit in enumerate(zbits):
        arrived = swap(stacked(held), bit)
        parts.append((arrived, [(1 << order) + r for r in range(1 << order)]))
        held = held + [arrived]
    note(own, [(0, 0)])
    note(other, [(0, 1)])
    stages = [parts[:2]] + [[part] for part in parts[2:]]
    for number, stage in enumerate(stages):
        fresh = stage[1:] if number == 0 else stage
        for piece, zs in fresh:
            note(piece, [(2 * z, 0) for z in zs])
        every = [z for _, zs in stage for z in zs]
        new = [z for _, zs in fresh for z in zs]
        if groups_first:
            crossed = []
            if fresh:
                crossed = [swap_x(stacked([piece for piece, _ in fresh]))]
                note(crossed[0], [(2 * z, 1) for z in new])
            sent = [piece for piece, _ in stage]
            entries = [(2 * z + 1, 0) for z in every]
            if number == 0:
                sent.append(other)
                entries.append((1, 1))
            entries += [(2 * z + 1, 1) for z in new]
            note(swap(stacked(sent + crossed), 1), entries)
        else:
            across = swap(stacked([piece for piece, _ in stage]), 1)
            note(across, [(2 * z + 1, 0) for z in every])
            both = swap_x(stacked([piece for piece, _ in fresh] + [across]))
            note(both, [(2 * z, 1) for z in new] + [(2 * z + 1, 1) for z in every])
    return pieces, table


def assemble(scratch, refs, table, starts, first, rows):
    for at, (piece, offset, _, _) in enumerate(table):
        start = pl.multiple_of(starts[first + at], rows)
        scratch[pl.ds(start, rows), :] = refs[piece][offset : offset + rows, :]


def table_starts(table, rows, chip, sent_core):
    flips = jnp.asarray([entry[2] for entry in table], jnp.int32)
    others = jnp.asarray([entry[3] for entry in table], jnp.int32)
    return (((chip ^ flips) * CORES) + (sent_core ^ others)) * rows


def dot(a, b):
    return lax.dot_general(a, b, (((1,), (0,)), ((), ())), preferred_element_type=F32)


def dot_tt(a, b):
    return lax.dot_general(a, b, (((1,), (1,)), ((), ())), preferred_element_type=F32)


def dot_outer(a, b):
    return lax.dot_general(a, b, (((0,), (0,)), ((), ())), preferred_element_type=F32)


def whole(shape):
    return pl.BlockSpec(shape, lambda *ids: (0,) * len(shape))


def block0(shape):
    return pl.BlockSpec((1, *shape), lambda i, *_: (i,) + (0,) * len(shape))


def params(**kw):
    return pltpu.CompilerParams(dimension_semantics=("arbitrary",), vmem_limit_bytes=60 << 20, **kw)


def keys_values_kernel(ktable, vtable, nk, rows, heads, starts, x, *refs):
    kp, refs = refs[:nk], refs[nk:]
    k_out, v_out, span_out, dev_out, total, wk, wv = refs[-7:]
    vp = refs[:-7]
    step = pl.program_id(0)

    @pl.when(step == 0)
    def _():
        assemble(wk, kp, ktable, starts, 0, rows)
        assemble(wv, vp, vtable, starts, len(ktable), rows)

    tokens = x[0]
    k = dot(tokens, wk[...]).astype(BF16)
    v = dot(tokens, wv[...]).astype(BF16)
    k_out[0] = k
    v_out[0] = v
    for h in range(heads):
        cols = slice(h * HEAD, (h + 1) * HEAD)
        device_sum = None
        for c in range(k.shape[0] // SPAN):
            span = slice(c * SPAN, (c + 1) * SPAN)
            state = dot_outer(k[span, cols], v[span, cols])
            span_out[0, c, h] = state.astype(BF16)
            device_sum = state if device_sum is None else device_sum + state
        dev_out[0, h] = device_sum.astype(BF16)

        @pl.when(step == 0)
        def _():
            total[h] = device_sum

        @pl.when(step > 0)
        def _():
            total[h] = total[h] + device_sum


def queries_kernel(qtable, rows, heads, levels, local_bits, starts, x, k, v, spans, other, scale, *refs):
    q_out, part_out, wq = refs[-3:]
    qp = refs[:-3]

    @pl.when(pl.program_id(0) == 0)
    def _():
        assemble(wq, qp, qtable, starts, 0, rows)

    q = dot(x[0], wq[...]).astype(BF16)
    q_out[0] = q
    row = lax.broadcasted_iota(jnp.int32, (SPAN, SPAN), 0)
    col = lax.broadcasted_iota(jnp.int32, (SPAN, SPAN), 1)
    apart = row ^ col
    causal = row >= col
    for c in range(q.shape[0] // SPAN):
        span = slice(c * SPAN, (c + 1) * SPAN)
        for h in range(heads):
            cols = slice(h * HEAD, (h + 1) * HEAD)

            def weight(level):
                at = h * levels + level
                return scale[0, span, at : at + 1]

            mixing = jnp.broadcast_to(weight(0), (SPAN, SPAN))
            for level in range(1, CBITS + 1):
                mixing = jnp.where(apart >= 1 << (level - 1), weight(level), mixing)
            qh = q[span, cols]
            scores = dot_tt(qh, k[0, span, cols])
            probs = jnp.where(causal, scores * mixing, 0.0).astype(BF16)
            out = dot(probs, v[0, span, cols])
            for b in range(1, local_bits + 1):
                half = 1 << (b - 1)
                if c & half:
                    base = (c >> b) << b
                    bucket = spans[0, base, h]
                    for more in range(1, half):
                        bucket = (bucket.astype(F32) + spans[0, base + more, h].astype(F32)).astype(BF16)
                    out = out + dot(qh, bucket) * weight(CBITS + b)
            out = out + dot(qh, other[0, h]) * weight(CBITS + local_bits + 1)
            part_out[0, span, cols] = out


def reads_kernel(heads, levels, first, q, part, scale, *refs):
    buckets, out = refs[:-1], refs[-1]
    for h in range(heads):
        cols = slice(h * HEAD, (h + 1) * HEAD)
        qh = q[0, :, cols]
        value = part[0, :, cols]
        for at, bucket in enumerate(buckets):
            col = h * levels + first + at
            value = value + dot(qh, bucket[h]) * scale[0, :, col : col + 1]
        out[0, :, cols] = value.astype(BF16)


def rows_kernel(table, rows, starts, *refs):
    assemble(refs[-1], refs[:-1], table, starts, 0, rows)


def output_kernel(core, mine, theirs, w_mine, w_theirs, out):
    depth = mine.shape[0]
    me = core[0]
    low = pl.multiple_of(me * depth, depth)
    high = pl.multiple_of((1 - me) * depth, depth)

    def write(w):
        out[...] = (dot(mine[...], w[pl.ds(low, depth), :]) + dot(theirs[...], w[pl.ds(high, depth), :])).astype(BF16)

    @pl.when(pl.program_id(0) == 0)
    def _():
        write(w_mine)

    @pl.when(pl.program_id(0) == 1)
    def _():
        write(w_theirs)


def prefetch_call(kernel, grid, in_specs, out_specs, out_shape, scratch, flops, name):
    return pl.pallas_call(
        kernel,
        grid_spec=pltpu.PrefetchScalarGridSpec(
            num_scalar_prefetch=1, grid=grid, in_specs=in_specs, out_specs=out_specs, scratch_shapes=scratch
        ),
        out_shape=out_shape,
        compiler_params=params(),
        cost_estimate=pl.CostEstimate(flops=flops, bytes_accessed=8 << 20, transcendentals=0),
        name=name,
    )


def on_device(tokens, w_qkv, w_out, level_weight):
    seq_bits = lax.axis_size("seq").bit_length() - 1
    device = lax.axis_index("seq")
    core, chip = device % CORES, device // CORES
    sent_core = lax.axis_index("group") % 2
    zbits = list(range(2, seq_bits))
    toks, width = tokens.shape
    levels = level_weight.shape[0]
    heads = HEADS // CORES
    cols = heads * HEAD
    head_cols = HEADS * HEAD
    local_bits = (toks // SPAN).bit_length() - 1
    mine_sent = core == sent_core

    def split_rows(pick):
        mine = pick(core)
        arrived = swap(pick(1 - core), 0)
        return jnp.where(mine_sent, mine, arrived), jnp.where(mine_sent, arrived, mine)

    rows = w_qkv.shape[0]

    def qkv_cols(which):
        return lambda c: lax.dynamic_slice(w_qkv, (0, which * head_cols + c * cols), (rows, cols))

    k_own, k_other = split_rows(qkv_cols(1))
    v_own, v_other = split_rows(qkv_cols(2))
    kp, ktable = gather_rows(k_own, k_other, zbits, False)
    vp, vtable = gather_rows(v_own, v_other, zbits, True)
    x = jnp.stack([tokens, swap(tokens, 0)])

    own_w = lax.dynamic_slice(level_weight, (0, core * heads, 0), (levels, heads, toks))
    far_w = swap(lax.dynamic_slice(level_weight, (0, (1 - core) * heads, 0), (levels, heads, toks)), 0)
    gains = [1.0 / math.sqrt(HEAD * max(1, 2 ** (n - 1))) for n in range(CBITS + 1)]
    gains += [1.0 / math.sqrt(SPAN * 2 ** (b - 1) * HEAD) for b in range(1, levels - CBITS)]
    first_bit = CBITS + 1 + local_bits
    shifts = jnp.asarray([max(0, n - first_bit) for n in range(levels)], jnp.int32)
    always = jnp.asarray([n < first_bit for n in range(levels)])
    block_device = jnp.stack([device, device ^ 1])
    on = jnp.where(always[None], 1, (block_device[:, None] >> shifts[None]) & 1).astype(F32)
    on = on * jnp.asarray(gains, F32)[None]
    scale = jnp.stack([own_w, far_w]) * on[:, :, None, None]
    scale = jnp.transpose(scale, (0, 3, 2, 1)).reshape(2, toks, heads * levels)

    starts = jnp.concatenate(
        [table_starts(ktable, rows, chip, sent_core), table_starts(vtable, rows, chip, sent_core)]
    )
    count = toks // SPAN
    sd = jax.ShapeDtypeStruct
    act = sd((2, toks, cols), BF16)
    k, v, spans, dev, total = prefetch_call(
        functools.partial(keys_values_kernel, ktable, vtable, len(kp), rows, heads),
        (2,),
        [block0((toks, width))] + [whole(p.shape) for p in kp + vp],
        [
            block0((toks, cols)),
            block0((toks, cols)),
            block0((count, heads, HEAD, HEAD)),
            block0((heads, HEAD, HEAD)),
            whole((heads, HEAD, HEAD)),
        ],
        [
            act,
            act,
            sd((2, count, heads, HEAD, HEAD), BF16),
            sd((2, heads, HEAD, HEAD), BF16),
            sd((heads, HEAD, HEAD), F32),
        ],
        [pltpu.VMEM((width, cols), BF16), pltpu.VMEM((width, cols), BF16)],
        2 * 2 * toks * width * 2 * cols,
        "keys_values",
    )(starts, x, *kp, *vp)

    buckets = []
    for bit in range(1, seq_bits):
        arrived = swap(total.astype(BF16), bit)
        buckets.append(arrived)
        total = total + arrived.astype(F32)

    q_own, q_other = split_rows(qkv_cols(0))
    qp, qtable = gather_rows(q_own, q_other, zbits, False)
    q, part = prefetch_call(
        functools.partial(queries_kernel, qtable, rows, heads, levels, local_bits),
        (2,),
        [
            block0((toks, width)),
            block0((toks, cols)),
            block0((toks, cols)),
            block0((count, heads, HEAD, HEAD)),
            pl.BlockSpec((1, heads, HEAD, HEAD), lambda i, *_: (1 - i, 0, 0, 0)),
            block0((toks, heads * levels)),
        ]
        + [whole(p.shape) for p in qp],
        [block0((toks, cols)), block0((toks, cols))],
        [act, sd((2, toks, cols), F32)],
        [pltpu.VMEM((width, cols), BF16)],
        2 * 2 * toks * width * cols,
        "queries",
    )(table_starts(qtable, rows, chip, sent_core), x, k, v, spans, dev, scale, *qp)

    out_rows, out_width = w_out.shape
    out_cols = out_width // CORES
    o_own, o_other = split_rows(lambda c: lax.dynamic_slice(w_out, (0, c * out_cols), (out_rows, out_cols)))
    op, otable = gather_rows(o_own, o_other, zbits, True)
    w_mine = prefetch_call(
        functools.partial(rows_kernel, otable, out_rows),
        (1,),
        [whole(p.shape) for p in op],
        whole((head_cols, out_cols)),
        sd((head_cols, out_cols), BF16),
        [],
        1 << 20,
        "out_rows",
    )(table_starts(otable, out_rows, chip, sent_core), *op)
    w_theirs = swap(w_mine, 0)

    attended = pl.pallas_call(
        functools.partial(reads_kernel, heads, levels, first_bit + 1),
        grid=(2,),
        in_specs=[block0((toks, cols)), block0((toks, cols)), block0((toks, heads * levels))]
        + [whole((heads, HEAD, HEAD))] * len(buckets),
        out_specs=block0((toks, cols)),
        out_shape=act,
        compiler_params=params(),
        cost_estimate=pl.CostEstimate(flops=1 << 30, bytes_accessed=8 << 20, transcendentals=0),
        name="reads",
    )(q, part, scale, *buckets)

    mine = attended[0]
    theirs = swap(attended[1], 0)
    return prefetch_call(
        output_kernel,
        (2,),
        [whole(mine.shape), whole(mine.shape), whole(w_mine.shape), whole(w_mine.shape)],
        pl.BlockSpec((toks, out_cols), lambda j, c: (0, jnp.where(j == 0, c[0], 1 - c[0]))),
        sd((toks, out_width), BF16),
        [],
        2 * toks * head_cols * out_width,
        "output",
    )(core.reshape(1).astype(jnp.int32), mine, theirs, w_mine, w_theirs)


def solution(mesh):
    return jax.shard_map(
        on_device,
        mesh=mesh,
        in_specs=(
            P(("group", "seq"), None),
            P("seq", None),
            P("seq", None),
            P(None, None, ("group", "seq")),
        ),
        out_specs=P(("group", "seq"), None),
        check_vma=False,
    )
```

```python
import functools
import math

import jax
import jax.numpy as jnp
from jax import lax
from jax.experimental import pallas as pl
from jax.experimental.pallas import tpu as pltpu
from jax.sharding import PartitionSpec as P


HEADS = 4
HEAD = 256
SPAN = 256
CBITS = 8
CORES = 2
F32 = jnp.float32
BF16 = jnp.bfloat16


def swap(value, bit):
    mask = 1 << bit
    return lax.ppermute(value, "seq", [(i, i ^ mask) for i in range(lax.axis_size("seq"))])


def swap_crossed(value, bit):
    size = lax.axis_size("seq")
    pairs = [
        (g * size + i, g * size + (i ^ (1 << bit) ^ (g % 2)))
        for g in range(lax.axis_size("group"))
        for i in range(size)
    ]
    return lax.ppermute(value, ("group", "seq"), pairs)


def swap_x(value):
    return lax.ppermute(value, "group", [(i, i ^ 1) for i in range(lax.axis_size("group"))])


OWN, OTHER, MINE, FAR = range(4)


def gather_rows(first, mine, arrived, zbits, turn):
    pieces = [(mine, 0, MINE), (arrived, 0, FAR)]
    across = swap_crossed(first, 1)
    pieces.append((across, 1, OWN))
    pieces.append((swap_x(across), 1, OTHER))
    held = []
    for bit in reversed(zbits):
        flip = 1 << (bit - 1)
        got = [(swap_crossed(first, bit), flip)]
        for piece, before in held:
            got.append((swap(piece, bit), before ^ flip))
        held += got
    for at, (piece, flip) in enumerate(held):
        side = swap_x(piece)
        across = swap(piece, 1)
        if (at + turn) % 2:
            corner = swap_x(across)
        else:
            corner = swap(side, 1)
        pieces += [(piece, flip, OWN), (side, flip, OTHER), (across, flip ^ 1, OWN), (corner, flip ^ 1, OTHER)]
    return pieces


def first_rows(pieces, rows, device, sent_core):
    core, chip = device % CORES, device // CORES
    flips = jnp.asarray([piece[1] for piece in pieces], jnp.int32)
    halves = jnp.asarray([piece[2] for piece in pieces], jnp.int32)
    return ((chip ^ flips) * CORES + (jnp.where(halves < MINE, sent_core, core) ^ (halves & 1))) * rows


def split_kernel(parts, width, *refs):
    sources, outs = refs[:-3], refs[-3:]
    core = lax.axis_index("seq") % CORES
    sent_core = core ^ (lax.axis_index("group") % 2)
    for out, half in zip(outs, (sent_core, core, 1 - core)):
        row = 0
        for source, offset, stride in parts:
            ref = sources[source]
            start = pl.multiple_of(offset + half * stride, width)
            out[row : row + ref.shape[0], :] = ref[:, pl.ds(start, width)]
            row += ref.shape[0]


def row_copies(dst, refs, offset, cols, starts, rows, sem, first, base=0):
    copies = []
    for at, ref in enumerate(refs):
        start = pl.multiple_of(starts[base + at], rows)
        copies.append(
            pltpu.make_async_copy(
                ref.at[pl.ds(offset, rows), :], dst.at[pl.ds(start, rows), cols], sem.at[first + at]
            )
        )
    return copies


def dot(a, b):
    return lax.dot_general(a, b, (((1,), (0,)), ((), ())), preferred_element_type=F32)


def dot_tt(a, b):
    return lax.dot_general(a, b, (((1,), (1,)), ((), ())), preferred_element_type=F32)


def dot_outer(a, b):
    return lax.dot_general(a, b, (((0,), (0,)), ((), ())), preferred_element_type=F32)


def keys_values_kernel(n, rows, heads, starts, xa, xb, scale, *refs):
    del scale
    pieces = refs[:n]
    ka, kb, va, vb, da, db, sent, wk, wv, x, sem, xsem = refs[n:]
    everything = slice(None)
    vcopies = row_copies(wv, pieces, 0, everything, starts, rows, sem, 0)
    kcopies = row_copies(wk, pieces, rows, everything, starts, rows, sem, n)
    xcopies = [pltpu.make_async_copy(src, x.at[i], xsem.at[i]) for i, src in enumerate((xa, xb))]
    xcopies[0].start()
    for copy in kcopies + vcopies:
        copy.start()
    xcopies[1].start()
    xcopies[0].wait()
    for copy in kcopies:
        copy.wait()
    sums = [None] * heads
    for i, (k_out, v_out) in enumerate(((ka, va), (kb, vb))):
        if i:
            xcopies[i].wait()
        k = dot(x[i], wk[...]).astype(BF16)
        k_out[...] = k
        if i == 0:
            for copy in vcopies:
                copy.wait()
        v = dot(x[i], wv[...]).astype(BF16)
        v_out[...] = v
        for h in range(heads):
            cols = slice(h * HEAD, (h + 1) * HEAD)
            state = dot_outer(k[:, cols], v[:, cols])
            (da, db)[i][h] = state.astype(BF16)
            sums[h] = state if i == 0 else sums[h] + state
    for h in range(heads):
        sent[h] = sums[h].astype(BF16)


def attend_kernel(which, n, nb, rows, out_rows, heads, levels, local_bits, starts, x_hbm, k, v, other, scale, *refs):
    buckets, pieces, refs = refs[:nb], refs[nb : nb + n], refs[nb + n :]
    if which:
        out, w_out, wq, x, sem, xsem, w, wsem = refs
    else:
        out, wq, x, sem, xsem = refs
    xcopy = pltpu.make_async_copy(x_hbm, x, xsem.at[0])
    xcopy.start()
    copies = row_copies(wq, pieces, 0, slice(None), starts, rows, sem, 0)
    for copy in copies:
        copy.start()
    moves = []
    if which:
        width = pieces[0].shape[1]
        for part in range(w.shape[1] // width):
            cols_of = pl.ds(part * width, width)
            moves += row_copies(w, pieces, rows + part * out_rows, cols_of, starts, out_rows, wsem, len(moves), n)
        for move in moves:
            move.start()
    row = lax.broadcasted_iota(jnp.int32, (SPAN, SPAN), 0)
    col = lax.broadcasted_iota(jnp.int32, (SPAN, SPAN), 1)
    apart = row ^ col
    causal = row >= col
    xcopy.wait()
    for copy in copies:
        copy.wait()
    q = dot(x[...], wq[...]).astype(BF16)
    store = None
    if which:
        for move in moves:
            move.wait()
        store = pltpu.make_async_copy(w, w_out, xsem.at[1])
        store.start()
    first = CBITS + local_bits + 1
    for h in range(heads):
        cols = slice(h * HEAD, (h + 1) * HEAD)
        states = []
        for c in range(q.shape[0] // SPAN):
            span = slice(c * SPAN, (c + 1) * SPAN)

            def weight(level):
                at = h * levels + level
                return scale[which, span, at : at + 1]

            mixing = jnp.broadcast_to(weight(0), (SPAN, SPAN))
            for level in range(1, CBITS + 1):
                mixing = jnp.where(apart >= 1 << (level - 1), weight(level), mixing)
            qh, kh, vh = q[span, cols], k[span, cols], v[span, cols]
            probs = jnp.where(causal, dot_tt(qh, kh) * mixing, 0.0).astype(BF16)
            value = dot(probs, vh)
            states.append(dot_outer(kh, vh) if c + 1 < q.shape[0] // SPAN else None)
            for b in range(1, local_bits + 1):
                half = 1 << (b - 1)
                if c & half:
                    base = (c >> b) << b
                    bucket = sum(states[base + 1 : base + half], states[base])
                    value = value + dot(qh, bucket.astype(BF16)) * weight(CBITS + b)
            for at, bucket in enumerate((other, *buckets)):
                value = value + dot(qh, bucket[h]) * weight(first + at)
            out[span, cols] = value.astype(BF16)
    if which:
        store.wait()


def output_kernel(width, core_ref, mine, theirs, w_mine, w_theirs, out, w, block, wsem, osem):
    depth = mine.shape[1]
    core = core_ref[0]
    parts = w_mine.shape[1] // width
    loads, stores = [], []
    for side, src in enumerate((w_mine, w_theirs)):
        for part in range(parts):
            at = side * parts + part
            loads.append(pltpu.make_async_copy(src.at[:, pl.ds(part * width, width)], w.at[at], wsem.at[at]))
            loads[-1].start()
    low = pl.multiple_of(core * depth, depth)
    high = pl.multiple_of((1 - core) * depth, depth)
    for at, load in enumerate(loads):
        load.wait()
        value = dot(mine[...], w[at, pl.ds(low, depth), :]) + dot(theirs[...], w[at, pl.ds(high, depth), :])
        block[at] = value.astype(BF16)
        half = core if at < parts else 1 - core
        start = pl.multiple_of((half * parts + at % parts) * width, width)
        stores.append(pltpu.make_async_copy(block.at[at], out.at[:, pl.ds(start, width)], osem.at[at]))
        stores[-1].start()
    for store in stores:
        store.wait()


ANY = pl.BlockSpec(memory_space=pl.ANY)


def whole(shape):
    return pl.BlockSpec(shape, lambda *ids: (0,) * len(shape))


def call(kernel, in_specs, out_specs, out_shape, scratch, flops, grid=(1,)):
    return pl.pallas_call(
        kernel,
        grid_spec=pltpu.PrefetchScalarGridSpec(
            num_scalar_prefetch=1, grid=grid, in_specs=in_specs, out_specs=out_specs, scratch_shapes=scratch
        ),
        out_shape=out_shape,
        compiler_params=pltpu.CompilerParams(dimension_semantics=("arbitrary",), vmem_limit_bytes=60 << 20),
        cost_estimate=pl.CostEstimate(flops=flops, bytes_accessed=8 << 20, transcendentals=0),
    )


def on_device(tokens, w_qkv, w_out, level_weight):
    seq_bits = lax.axis_size("seq").bit_length() - 1
    device = lax.axis_index("seq")
    core = device % CORES
    odd_group = lax.axis_index("group") % 2
    sent_core = core ^ odd_group
    zbits = list(range(2, seq_bits))
    toks, width = tokens.shape
    levels = level_weight.shape[0]
    heads = HEADS // CORES
    cols = heads * HEAD
    head_cols = HEADS * HEAD
    local_bits = (toks // SPAN).bit_length() - 1
    rows = w_qkv.shape[0]
    out_rows, out_width = w_out.shape
    out_cols = out_width // CORES
    sd = jax.ShapeDtypeStruct

    def split(sources, parts):
        shape = (sum(sources[part[0]].shape[0] for part in parts), cols)
        first, mine, far = pl.pallas_call(
            functools.partial(split_kernel, parts, cols),
            out_shape=[sd(shape, BF16)] * 3,
            cost_estimate=pl.CostEstimate(flops=1 << 20, bytes_accessed=2 << 20, transcendentals=0),
        )(*sources)
        return first, mine, swap(far, 0)

    kv_split = split((w_qkv,), ((0, 2 * head_cols, cols), (0, head_cols, cols)))
    out_parts = out_cols // cols
    qo_split = split((w_qkv, w_out), ((0, 0, cols),) + tuple((1, n * cols, out_cols) for n in range(out_parts)))
    far_tokens = swap(tokens, 0)

    own_w = lax.dynamic_slice(level_weight, (0, core * heads, 0), (levels, heads, toks))
    far_w = swap(lax.dynamic_slice(level_weight, (0, (1 - core) * heads, 0), (levels, heads, toks)), 0)
    gains = [1.0 / math.sqrt(HEAD * max(1, 2 ** (n - 1))) for n in range(CBITS + 1)]
    gains += [1.0 / math.sqrt(SPAN * 2 ** (b - 1) * HEAD) for b in range(1, levels - CBITS)]
    first_bit = CBITS + 1 + local_bits
    shifts = jnp.asarray([max(0, n - first_bit) for n in range(levels)], jnp.int32)
    always = jnp.asarray([n < first_bit for n in range(levels)])
    block_device = jnp.stack([device, device ^ 1])
    on = jnp.where(always[None], 1, (block_device[:, None] >> shifts[None]) & 1).astype(F32)
    on = on * jnp.asarray(gains, F32)[None]
    scale = jnp.stack([own_w, far_w]) * on[:, :, None, None]
    scale = jnp.transpose(scale, (0, 3, 2, 1)).reshape(2, toks, heads * levels)

    kvp = gather_rows(*kv_split, zbits, 0)
    qop = gather_rows(*qo_split, zbits, 1)

    act = sd((toks, cols), BF16)
    act_spec = whole((toks, cols))
    state_spec = whole((heads, HEAD, HEAD))
    state = sd((heads, HEAD, HEAD), BF16)
    ka, kb, va, vb, da, db, total = call(
        functools.partial(keys_values_kernel, len(kvp), rows, heads),
        [ANY] * (3 + len(kvp)),
        [act_spec] * 4 + [state_spec] * 3,
        [act] * 4 + [state] * 3,
        [
            pltpu.VMEM((width, cols), BF16),
            pltpu.VMEM((width, cols), BF16),
            pltpu.VMEM((2, toks, width), BF16),
            pltpu.SemaphoreType.DMA((2 * len(kvp),)),
            pltpu.SemaphoreType.DMA((2,)),
        ],
        2 * 2 * toks * width * 2 * cols,
    )(first_rows(kvp, rows, device, sent_core), tokens, far_tokens, scale, *(piece[0] for piece in kvp))

    buckets = []
    for bit in range(1, seq_bits):
        arrived = swap(total, bit)
        buckets.append(arrived)
        total = (total.astype(F32) + arrived.astype(F32)).astype(BF16)

    def attend(which, x, k, v, other):
        specs, shapes = [act_spec], [act]
        scratch = [
            pltpu.VMEM((width, cols), BF16),
            pltpu.VMEM((toks, width), BF16),
            pltpu.SemaphoreType.DMA((len(qop),)),
            pltpu.SemaphoreType.DMA((2,)),
        ]
        if which:
            specs.append(ANY)
            shapes.append(sd((head_cols, out_cols), BF16))
            scratch += [pltpu.VMEM((head_cols, out_cols), BF16), pltpu.SemaphoreType.DMA((out_parts * len(qop),))]
        return call(
            functools.partial(
                attend_kernel, which, len(qop), len(buckets), rows, out_rows, heads, levels, local_bits
            ),
            [ANY] + [act_spec] * 2 + [state_spec] + [whole(scale.shape)] + [state_spec] * len(buckets)
            + [ANY] * len(qop),
            specs,
            shapes,
            scratch,
            2 * toks * width * cols,
        )(
            jnp.concatenate(
                [first_rows(qop, rows, device, sent_core), first_rows(qop, out_rows, device, sent_core)]
            ),
            x, k, v, other, scale, *buckets, *(piece[0] for piece in qop),
        )

    far_part, w_mine = attend(1, far_tokens, kb, vb, da)
    theirs = swap(far_part, 0)
    w_theirs = swap(w_mine, 0)
    (mine,) = attend(0, tokens, ka, va, db)
    n_blocks = CORES * out_parts
    return call(
        functools.partial(output_kernel, cols),
        [act_spec, act_spec, ANY, ANY],
        ANY,
        sd((toks, out_width), BF16),
        [
            pltpu.VMEM((n_blocks, head_cols, cols), BF16),
            pltpu.VMEM((n_blocks, toks, cols), BF16),
            pltpu.SemaphoreType.DMA((n_blocks,)),
            pltpu.SemaphoreType.DMA((n_blocks,)),
        ],
        2 * toks * head_cols * out_width,
    )(core.reshape(1).astype(jnp.int32), mine, theirs, w_mine, w_theirs)


def solution(mesh):
    return jax.shard_map(
        on_device,
        mesh=mesh,
        in_specs=(
            P(("group", "seq"), None),
            P("seq", None),
            P("seq", None),
            P(None, None, ("group", "seq")),
        ),
        out_specs=P(("group", "seq"), None),
        check_vma=False,
    )
```

```python
import functools
import math

import jax
import jax.numpy as jnp
from jax import lax
from jax.experimental import pallas as pl
from jax.experimental.pallas import tpu as pltpu
from jax.sharding import PartitionSpec as P


HEADS = 4
HEAD = 256
SPAN = 256
CBITS = 8
CORES = 2
F32 = jnp.float32
BF16 = jnp.bfloat16


def swap(value, bit):
    mask = 1 << bit
    return lax.ppermute(value, "seq", [(i, i ^ mask) for i in range(lax.axis_size("seq"))])


def swap_crossed(value, bit):
    size = lax.axis_size("seq")
    pairs = [
        (g * size + i, g * size + (i ^ (1 << bit) ^ (g % 2)))
        for g in range(lax.axis_size("group"))
        for i in range(size)
    ]
    return lax.ppermute(value, ("group", "seq"), pairs)


def swap_x(value):
    return lax.ppermute(value, "group", [(i, i ^ 1) for i in range(lax.axis_size("group"))])


OWN, OTHER, MINE, FAR = range(4)


def gather_rows(first, mine, arrived, zbits, turn):
    pieces = [(mine, 0, MINE), (arrived, 0, FAR)]
    across = swap_crossed(first, 1)
    pieces.append((across, 1, OWN))
    pieces.append((swap_x(across), 1, OTHER))
    held = []
    for bit in reversed(zbits):
        flip = 1 << (bit - 1)
        got = [(swap_crossed(first, bit), flip)]
        for piece, before in held:
            got.append((swap(piece, bit), before ^ flip))
        held += got
    for at, (piece, flip) in enumerate(held):
        side = swap_x(piece)
        across = swap(piece, 1)
        if (at + turn) % 2:
            corner = swap_x(across)
        else:
            corner = swap(side, 1)
        pieces += [(piece, flip, OWN), (side, flip, OTHER), (across, flip ^ 1, OWN), (corner, flip ^ 1, OTHER)]
    return pieces


def first_rows(pieces, rows, device, sent_core):
    core, chip = device % CORES, device // CORES
    flips = jnp.asarray([piece[1] for piece in pieces], jnp.int32)
    halves = jnp.asarray([piece[2] for piece in pieces], jnp.int32)
    return ((chip ^ flips) * CORES + (jnp.where(halves < MINE, sent_core, core) ^ (halves & 1))) * rows


def split_kernel(parts, width, *refs):
    sources, outs = refs[:-3], refs[-3:]
    core = lax.axis_index("seq") % CORES
    sent_core = core ^ (lax.axis_index("group") % 2)
    for out, half in zip(outs, (sent_core, core, 1 - core)):
        row = 0
        for source, offset, stride in parts:
            ref = sources[source]
            start = pl.multiple_of(offset + half * stride, width)
            out[row : row + ref.shape[0], :] = ref[:, pl.ds(start, width)]
            row += ref.shape[0]


def place_rows(dst, pieces, offset, cols, starts, base, rows):
    for at, piece in enumerate(pieces):
        start = pl.multiple_of(starts[base + at], rows)
        dst[pl.ds(start, rows), cols] = piece[offset : offset + rows, :]


def dot(a, b):
    return lax.dot_general(a, b, (((1,), (0,)), ((), ())), preferred_element_type=F32)


def dot_tt(a, b):
    return lax.dot_general(a, b, (((1,), (1,)), ((), ())), preferred_element_type=F32)


def dot_outer(a, b):
    return lax.dot_general(a, b, (((0,), (0,)), ((), ())), preferred_element_type=F32)


def keys_values_kernel(n, rows, heads, starts, xa, xb, scale, *refs):
    del scale
    pieces = refs[:n]
    ka, kb, va, vb, da, db, sent, wk, wv = refs[n:]
    everything = slice(None)
    place_rows(wk, pieces, rows, everything, starts, 0, rows)
    place_rows(wv, pieces, 0, everything, starts, 0, rows)
    sums = [None] * heads
    for i, (x, k_out, v_out, device_sum) in enumerate(((xa, ka, va, da), (xb, kb, vb, db))):
        k = dot(x[...], wk[...]).astype(BF16)
        k_out[...] = k
        v = dot(x[...], wv[...]).astype(BF16)
        v_out[...] = v
        for h in range(heads):
            cols = slice(h * HEAD, (h + 1) * HEAD)
            state = dot_outer(k[:, cols], v[:, cols])
            device_sum[h] = state.astype(BF16)
            sums[h] = state if i == 0 else sums[h] + state
    for h in range(heads):
        sent[h] = sums[h].astype(BF16)


def attend_kernel(which, n, nb, rows, out_rows, heads, levels, local_bits, starts, x, k, v, other, scale, *refs):
    buckets, pieces, refs = refs[:nb], refs[nb : nb + n], refs[nb + n :]
    out, wq = refs[0], refs[-1]
    place_rows(wq, pieces, 0, slice(None), starts, 0, rows)
    if which:
        w = refs[1]
        width = pieces[0].shape[1]
        for part in range(w.shape[1] // width):
            cols = slice(part * width, (part + 1) * width)
            place_rows(w, pieces, rows + part * out_rows, cols, starts, n, out_rows)
    row = lax.broadcasted_iota(jnp.int32, (SPAN, SPAN), 0)
    col = lax.broadcasted_iota(jnp.int32, (SPAN, SPAN), 1)
    apart = row ^ col
    causal = row >= col
    q = dot(x[...], wq[...]).astype(BF16)
    first = CBITS + local_bits + 1
    for h in range(heads):
        cols = slice(h * HEAD, (h + 1) * HEAD)
        states = []
        for c in range(q.shape[0] // SPAN):
            span = slice(c * SPAN, (c + 1) * SPAN)

            def weight(level):
                at = h * levels + level
                return scale[which, span, at : at + 1]

            mixing = jnp.broadcast_to(weight(0), (SPAN, SPAN))
            for level in range(1, CBITS + 1):
                mixing = jnp.where(apart >= 1 << (level - 1), weight(level), mixing)
            qh, kh, vh = q[span, cols], k[span, cols], v[span, cols]
            probs = jnp.where(causal, dot_tt(qh, kh) * mixing, 0.0).astype(BF16)
            value = dot(probs, vh)
            states.append(dot_outer(kh, vh) if c + 1 < q.shape[0] // SPAN else None)
            for b in range(1, local_bits + 1):
                half = 1 << (b - 1)
                if c & half:
                    base = (c >> b) << b
                    bucket = sum(states[base + 1 : base + half], states[base])
                    value = value + dot(qh, bucket.astype(BF16)) * weight(CBITS + b)
            for at, bucket in enumerate((other, *buckets)):
                value = value + dot(qh, bucket[h]) * weight(first + at)
            out[span, cols] = value.astype(BF16)


def output_kernel(width, core_ref, mine, theirs, w_mine, w_theirs, out, block, sem):
    depth = mine.shape[1]
    core = core_ref[0]
    parts = w_mine.shape[1] // width
    low = pl.multiple_of(core * depth, depth)
    high = pl.multiple_of((1 - core) * depth, depth)
    stores = []
    for side, w in enumerate((w_mine, w_theirs)):
        for part in range(parts):
            at = side * parts + part
            cols = slice(part * width, (part + 1) * width)
            value = dot(mine[...], w[pl.ds(low, depth), cols]) + dot(theirs[...], w[pl.ds(high, depth), cols])
            block[at] = value.astype(BF16)
            half = core if side == 0 else 1 - core
            start = pl.multiple_of((half * parts + part) * width, width)
            stores.append(pltpu.make_async_copy(block.at[at], out.at[:, pl.ds(start, width)], sem.at[at]))
            stores[-1].start()
    for store in stores:
        store.wait()


ANY = pl.BlockSpec(memory_space=pl.ANY)
SMALL = pl.BlockSpec(memory_space=pltpu.SMEM)
FAST = pl.BlockSpec(memory_space=pltpu.VMEM)


def call(kernel, operands, out_specs, out_shape, scratch, flops, room=24):
    return pl.pallas_call(
        kernel,
        in_specs=[SMALL] + [FAST] * (len(operands) - 1),
        out_specs=out_specs,
        out_shape=out_shape,
        scratch_shapes=scratch,
        compiler_params=pltpu.CompilerParams(vmem_limit_bytes=room << 20),
        cost_estimate=pl.CostEstimate(flops=flops, bytes_accessed=8 << 20, transcendentals=0),
    )(*operands)


def on_device(tokens, w_qkv, w_out, level_weight):
    seq_bits = lax.axis_size("seq").bit_length() - 1
    device = lax.axis_index("seq")
    core = device % CORES
    odd_group = lax.axis_index("group") % 2
    sent_core = core ^ odd_group
    zbits = list(range(2, seq_bits))
    toks, width = tokens.shape
    levels = level_weight.shape[0]
    heads = HEADS // CORES
    cols = heads * HEAD
    head_cols = HEADS * HEAD
    local_bits = (toks // SPAN).bit_length() - 1
    rows = w_qkv.shape[0]
    out_rows, out_width = w_out.shape
    out_cols = out_width // CORES
    sd = jax.ShapeDtypeStruct

    def split(sources, parts):
        shape = (sum(sources[part[0]].shape[0] for part in parts), cols)
        first, mine, far = pl.pallas_call(
            functools.partial(split_kernel, parts, cols),
            out_shape=[sd(shape, BF16)] * 3,
            cost_estimate=pl.CostEstimate(flops=1 << 20, bytes_accessed=2 << 20, transcendentals=0),
        )(*sources)
        return first, mine, swap(far, 0)

    kv_split = split((w_qkv,), ((0, 2 * head_cols, cols), (0, head_cols, cols)))
    out_parts = out_cols // cols
    qo_split = split((w_qkv, w_out), ((0, 0, cols),) + tuple((1, n * cols, out_cols) for n in range(out_parts)))
    far_tokens = swap(tokens, 0)

    own_w = lax.dynamic_slice(level_weight, (0, core * heads, 0), (levels, heads, toks))
    far_w = swap(lax.dynamic_slice(level_weight, (0, (1 - core) * heads, 0), (levels, heads, toks)), 0)
    gains = [1.0 / math.sqrt(HEAD * max(1, 2 ** (n - 1))) for n in range(CBITS + 1)]
    gains += [1.0 / math.sqrt(SPAN * 2 ** (b - 1) * HEAD) for b in range(1, levels - CBITS)]
    first_bit = CBITS + 1 + local_bits
    shifts = jnp.asarray([max(0, n - first_bit) for n in range(levels)], jnp.int32)
    always = jnp.asarray([n < first_bit for n in range(levels)])
    block_device = jnp.stack([device, device ^ 1])
    on = jnp.where(always[None], 1, (block_device[:, None] >> shifts[None]) & 1).astype(F32)
    on = on * jnp.asarray(gains, F32)[None]
    scale = jnp.stack([own_w, far_w]) * on[:, :, None, None]
    scale = jnp.transpose(scale, (0, 3, 2, 1)).reshape(2, toks, heads * levels)

    kvp = gather_rows(*kv_split, zbits, 0)
    qop = gather_rows(*qo_split, zbits, 1)

    act = sd((toks, cols), BF16)
    state = sd((heads, HEAD, HEAD), BF16)
    ka, kb, va, vb, da, db, total = call(
        functools.partial(keys_values_kernel, len(kvp), rows, heads),
        [first_rows(kvp, rows, device, sent_core), tokens, far_tokens, scale, *(piece[0] for piece in kvp)],
        [FAST] * 7,
        [act] * 4 + [state] * 3,
        [pltpu.VMEM((width, cols), BF16), pltpu.VMEM((width, cols), BF16)],
        2 * 2 * toks * width * 2 * cols,
    )

    buckets = []
    for bit in range(1, seq_bits):
        arrived = swap(total, bit)
        buckets.append(arrived)
        total = (total.astype(F32) + arrived.astype(F32)).astype(BF16)

    starts = jnp.concatenate(
        [first_rows(qop, rows, device, sent_core), first_rows(qop, out_rows, device, sent_core)]
    )

    def attend(which, x, k, v, other):
        shapes = [act] + [sd((head_cols, out_cols), BF16)] * which
        return call(
            functools.partial(
                attend_kernel, which, len(qop), len(buckets), rows, out_rows, heads, levels, local_bits
            ),
            [starts, x, k, v, other, scale, *buckets, *(piece[0] for piece in qop)],
            [FAST] * len(shapes),
            shapes,
            [pltpu.VMEM((width, cols), BF16)],
            2 * toks * width * cols,
        )

    far_part, w_mine = attend(1, far_tokens, kb, vb, da)
    theirs = swap(far_part, 0)
    w_theirs = swap(w_mine, 0)
    (mine,) = attend(0, tokens, ka, va, db)
    n_blocks = CORES * out_parts
    return call(
        functools.partial(output_kernel, cols),
        [core.reshape(1).astype(jnp.int32), mine, theirs, w_mine, w_theirs],
        ANY,
        sd((toks, out_width), BF16),
        [pltpu.VMEM((n_blocks, toks, cols), BF16), pltpu.SemaphoreType.DMA((n_blocks,))],
        2 * toks * head_cols * out_width,
    )


def solution(mesh):
    return jax.shard_map(
        on_device,
        mesh=mesh,
        in_specs=(
            P(("group", "seq"), None),
            P("seq", None),
            P("seq", None),
            P(None, None, ("group", "seq")),
        ),
        out_specs=P(("group", "seq"), None),
        check_vma=False,
    )
```

```python
import functools
import math

import jax
import jax.numpy as jnp
from jax import lax
from jax.experimental import pallas as pl
from jax.experimental.pallas import tpu as pltpu
from jax.sharding import PartitionSpec as P


HEADS = 4
HEAD = 256
SPAN = 256
CBITS = 8
CORES = 2
F32 = jnp.float32
BF16 = jnp.bfloat16


def swap(value, bit):
    mask = 1 << bit
    return lax.ppermute(value, "seq", [(i, i ^ mask) for i in range(lax.axis_size("seq"))])


def swap_crossed(value, bit, even=0):
    size = lax.axis_size("seq")
    pairs = [
        (g * size + i, g * size + (i ^ (1 << bit) ^ ((g + even) % 2)))
        for g in range(lax.axis_size("group"))
        for i in range(size)
    ]
    return lax.ppermute(value, ("group", "seq"), pairs)


def swap_x(value):
    return lax.ppermute(value, "group", [(i, i ^ 1) for i in range(lax.axis_size("group"))])


OWN, OTHER, MINE, FAR = range(4)


def gather_rows(first, second, mine, arrived, zbits, turn):
    pieces = [(mine, 0, MINE), (arrived, 0, FAR)]
    beside = swap_crossed(first, 1)
    pieces.append((beside, 1, OWN))
    pieces.append((swap_x(beside), 1, OTHER))
    held = []
    for bit in reversed(zbits):
        flip = 1 << (bit - 1)
        got = [(swap_crossed(first, bit), flip)]
        for piece, before in held:
            got.append((swap(piece, bit), before ^ flip))
        held += got
    for at, (piece, flip) in enumerate(held):
        if flip == 1 << (zbits[0] - 1):
            side = swap_crossed(second, zbits[0], 1)
            across = swap(beside, zbits[0])
        else:
            side = swap_x(piece)
            across = swap(piece, 1)
        if at in turn:
            corner = swap_x(across)
        else:
            corner = swap(side, 1)
        pieces += [(piece, flip, OWN), (side, flip, OTHER), (across, flip ^ 1, OWN), (corner, flip ^ 1, OTHER)]
    return pieces


def first_rows(pieces, rows, device, sent_core):
    core, chip = device % CORES, device // CORES
    flips = jnp.asarray([piece[1] for piece in pieces], jnp.int32)
    halves = jnp.asarray([piece[2] for piece in pieces], jnp.int32)
    return ((chip ^ flips) * CORES + (jnp.where(halves < MINE, sent_core, core) ^ (halves & 1))) * rows


def split_kernel(parts, width, *refs):
    sources, outs = refs[:-4], refs[-4:]
    core = lax.axis_index("seq") % CORES
    sent_core = core ^ (lax.axis_index("group") % 2)
    for out, half in zip(outs, (sent_core, 1 - sent_core, core, 1 - core)):
        row = 0
        for source, offset, stride in parts:
            ref = sources[source]
            start = pl.multiple_of(offset + half * stride, width)
            out[row : row + ref.shape[0], :] = ref[:, pl.ds(start, width)]
            row += ref.shape[0]


def place_rows(dst, pieces, offset, cols, starts, base, rows):
    for at, piece in enumerate(pieces):
        start = pl.multiple_of(starts[base + at], rows)
        dst[pl.ds(start, rows), cols] = piece[offset : offset + rows, :]


def dot(a, b):
    return lax.dot_general(a, b, (((1,), (0,)), ((), ())), preferred_element_type=F32)


def dot_tt(a, b):
    return lax.dot_general(a, b, (((1,), (1,)), ((), ())), preferred_element_type=F32)


def dot_outer(a, b):
    return lax.dot_general(a, b, (((0,), (0,)), ((), ())), preferred_element_type=F32)


def keys_values_kernel(n, rows, heads, starts, xa, xb, scale, *refs):
    del scale
    pieces = refs[:n]
    ka, kb, va, vb, da, db, sent, wk, wv = refs[n:]
    everything = slice(None)
    place_rows(wk, pieces, rows, everything, starts, 0, rows)
    place_rows(wv, pieces, 0, everything, starts, 0, rows)
    sums = [None] * heads
    for i, (x, k_out, v_out, device_sum) in enumerate(((xa, ka, va, da), (xb, kb, vb, db))):
        k = dot(x[...], wk[...]).astype(BF16)
        k_out[...] = k
        v = dot(x[...], wv[...]).astype(BF16)
        v_out[...] = v
        for h in range(heads):
            cols = slice(h * HEAD, (h + 1) * HEAD)
            state = dot_outer(k[:, cols], v[:, cols])
            device_sum[h] = state.astype(BF16)
            sums[h] = state if i == 0 else sums[h] + state
    for h in range(heads):
        sent[h] = sums[h].astype(BF16)


def attend_kernel(which, n, nb, rows, out_rows, heads, levels, local_bits, starts, x, k, v, other, scale, *refs):
    buckets, pieces, refs = refs[:nb], refs[nb : nb + n], refs[nb + n :]
    out, q_out, wq = refs[0], refs[1], refs[-1]
    place_rows(wq, pieces, 0, slice(None), starts, 0, rows)
    if which:
        w = refs[2]
        width = pieces[0].shape[1]
        for part in range(w.shape[1] // width):
            cols = slice(part * width, (part + 1) * width)
            place_rows(w, pieces, rows + part * out_rows, cols, starts, n, out_rows)
    row = lax.broadcasted_iota(jnp.int32, (SPAN, SPAN), 0)
    col = lax.broadcasted_iota(jnp.int32, (SPAN, SPAN), 1)
    apart = row ^ col
    causal = row >= col
    q = dot(x[...], wq[...]).astype(BF16)
    q_out[...] = q
    first = CBITS + local_bits + 1
    for h in range(heads):
        cols = slice(h * HEAD, (h + 1) * HEAD)
        states = []
        for c in range(q.shape[0] // SPAN):
            span = slice(c * SPAN, (c + 1) * SPAN)

            def weight(level):
                at = h * levels + level
                return scale[which, span, at : at + 1]

            mixing = jnp.broadcast_to(weight(0), (SPAN, SPAN))
            for level in range(1, CBITS + 1):
                mixing = jnp.where(apart >= 1 << (level - 1), weight(level), mixing)
            qh, kh, vh = q[span, cols], k[span, cols], v[span, cols]
            probs = jnp.where(causal, dot_tt(qh, kh) * mixing, 0.0).astype(BF16)
            value = dot(probs, vh)
            states.append(dot_outer(kh, vh) if c + 1 < q.shape[0] // SPAN else None)
            for b in range(1, local_bits + 1):
                half = 1 << (b - 1)
                if c & half:
                    base = (c >> b) << b
                    bucket = sum(states[base + 1 : base + half], states[base])
                    value = value + dot(qh, bucket.astype(BF16)) * weight(CBITS + b)
            for at, bucket in enumerate((other, *buckets)):
                value = value + dot(qh, bucket[h]) * weight(first + at)
            out[span, cols] = value


def reads_kernel(which, heads, levels, level, scale, part, q, bucket, out):
    for h in range(heads):
        cols = slice(h * HEAD, (h + 1) * HEAD)
        at = h * levels + level
        weight = scale[which, :, at : at + 1]
        out[:, cols] = (part[:, cols] + dot(q[:, cols], bucket[h]) * weight).astype(BF16)


def output_kernel(width, core_ref, mine, theirs, w_mine, w_theirs, out, block, sem):
    depth = mine.shape[1]
    core = core_ref[0]
    parts = w_mine.shape[1] // width
    low = pl.multiple_of(core * depth, depth)
    high = pl.multiple_of((1 - core) * depth, depth)
    stores = []
    for side, w in enumerate((w_mine, w_theirs)):
        for part in range(parts):
            at = side * parts + part
            cols = slice(part * width, (part + 1) * width)
            value = dot(mine[...], w[pl.ds(low, depth), cols]) + dot(theirs[...], w[pl.ds(high, depth), cols])
            block[at] = value.astype(BF16)
            half = core if side == 0 else 1 - core
            start = pl.multiple_of((half * parts + part) * width, width)
            stores.append(pltpu.make_async_copy(block.at[at], out.at[:, pl.ds(start, width)], sem.at[at]))
            stores[-1].start()
    for store in stores:
        store.wait()


ANY = pl.BlockSpec(memory_space=pl.ANY)
SMALL = pl.BlockSpec(memory_space=pltpu.SMEM)
FAST = pl.BlockSpec(memory_space=pltpu.VMEM)


def call(kernel, operands, out_specs, out_shape, scratch, flops, room=12):
    return pl.pallas_call(
        kernel,
        in_specs=[SMALL] + [FAST] * (len(operands) - 1),
        out_specs=out_specs,
        out_shape=out_shape,
        scratch_shapes=scratch,
        compiler_params=pltpu.CompilerParams(vmem_limit_bytes=room << 20),
        cost_estimate=pl.CostEstimate(flops=flops, bytes_accessed=8 << 20, transcendentals=0),
    )(*operands)


def on_device(tokens, w_qkv, w_out, level_weight):
    seq_bits = lax.axis_size("seq").bit_length() - 1
    device = lax.axis_index("seq")
    core = device % CORES
    odd_group = lax.axis_index("group") % 2
    sent_core = core ^ odd_group
    zbits = list(range(2, seq_bits))
    toks, width = tokens.shape
    levels = level_weight.shape[0]
    heads = HEADS // CORES
    cols = heads * HEAD
    head_cols = HEADS * HEAD
    local_bits = (toks // SPAN).bit_length() - 1
    rows = w_qkv.shape[0]
    out_rows, out_width = w_out.shape
    out_cols = out_width // CORES
    sd = jax.ShapeDtypeStruct

    def split(sources, parts):
        shape = (sum(sources[part[0]].shape[0] for part in parts), cols)
        first, second, mine, far = pl.pallas_call(
            functools.partial(split_kernel, parts, cols),
            out_shape=[sd(shape, BF16)] * 4,
            cost_estimate=pl.CostEstimate(flops=1 << 20, bytes_accessed=2 << 20, transcendentals=0),
        )(*sources)
        return first, second, mine, swap(far, 0)

    kv_split = split((w_qkv,), ((0, 2 * head_cols, cols), (0, head_cols, cols)))
    out_parts = out_cols // cols
    qo_split = split((w_qkv, w_out), ((0, 0, cols),) + tuple((1, n * cols, out_cols) for n in range(out_parts)))
    far_tokens = swap(tokens, 0)

    own_w = lax.dynamic_slice(level_weight, (0, core * heads, 0), (levels, heads, toks))
    far_w = swap(lax.dynamic_slice(level_weight, (0, (1 - core) * heads, 0), (levels, heads, toks)), 0)
    gains = [1.0 / math.sqrt(HEAD * max(1, 2 ** (n - 1))) for n in range(CBITS + 1)]
    gains += [1.0 / math.sqrt(SPAN * 2 ** (b - 1) * HEAD) for b in range(1, levels - CBITS)]
    first_bit = CBITS + 1 + local_bits
    shifts = jnp.asarray([max(0, n - first_bit) for n in range(levels)], jnp.int32)
    always = jnp.asarray([n < first_bit for n in range(levels)])
    block_device = jnp.stack([device, device ^ 1])
    on = jnp.where(always[None], 1, (block_device[:, None] >> shifts[None]) & 1).astype(F32)
    on = on * jnp.asarray(gains, F32)[None]
    scale = jnp.stack([own_w, far_w]) * on[:, :, None, None]
    scale = jnp.transpose(scale, (0, 3, 2, 1)).reshape(2, toks, heads * levels)

    kvp = gather_rows(*kv_split, zbits, (0,))
    qop = gather_rows(*qo_split, zbits, (0, 1))

    act = sd((toks, cols), BF16)
    state = sd((heads, HEAD, HEAD), BF16)
    ka, kb, va, vb, da, db, total = call(
        functools.partial(keys_values_kernel, len(kvp), rows, heads),
        [first_rows(kvp, rows, device, sent_core), tokens, far_tokens, scale, *(piece[0] for piece in kvp)],
        [FAST] * 7,
        [act] * 4 + [state] * 3,
        [pltpu.VMEM((width, cols), BF16), pltpu.VMEM((width, cols), BF16)],
        2 * 2 * toks * width * 2 * cols,
    )

    buckets = []
    for bit in range(1, seq_bits):
        arrived = swap(total, bit)
        buckets.append(arrived)
        total = (total.astype(F32) + arrived.astype(F32)).astype(BF16)

    starts = jnp.concatenate(
        [first_rows(qop, rows, device, sent_core), first_rows(qop, out_rows, device, sent_core)]
    )

    def attend(which, x, k, v, other):
        shapes = [sd((toks, cols), F32), act] + [sd((head_cols, out_cols), BF16)] * which
        return call(
            functools.partial(
                attend_kernel, which, len(qop), len(buckets) - 1, rows, out_rows, heads, levels, local_bits
            ),
            [starts, x, k, v, other, scale, *buckets[:-1], *(piece[0] for piece in qop)],
            [FAST] * len(shapes),
            shapes,
            [pltpu.VMEM((width, cols), BF16)],
            2 * toks * width * cols,
        )

    def read(which, part, q):
        return pl.pallas_call(
            functools.partial(reads_kernel, which, heads, levels, first_bit + seq_bits - 1),
            in_specs=[FAST] * 4,
            out_specs=FAST,
            out_shape=act,
            compiler_params=pltpu.CompilerParams(vmem_limit_bytes=8 << 20),
            cost_estimate=pl.CostEstimate(flops=1 << 28, bytes_accessed=2 << 20, transcendentals=0),
        )(scale, part, q, buckets[-1])

    far_part, far_q, w_mine = attend(1, far_tokens, kb, vb, da)
    w_theirs = swap(w_mine, 0)
    own_part, own_q = attend(0, tokens, ka, va, db)
    theirs = swap(read(1, far_part, far_q), 0)
    mine = read(0, own_part, own_q)
    n_blocks = CORES * out_parts
    return call(
        functools.partial(output_kernel, cols),
        [core.reshape(1).astype(jnp.int32), mine, theirs, w_mine, w_theirs],
        ANY,
        sd((toks, out_width), BF16),
        [pltpu.VMEM((n_blocks, toks, cols), BF16), pltpu.SemaphoreType.DMA((n_blocks,))],
        2 * toks * head_cols * out_width,
    )


def solution(mesh):
    return jax.shard_map(
        on_device,
        mesh=mesh,
        in_specs=(
            P(("group", "seq"), None),
            P("seq", None),
            P("seq", None),
            P(None, None, ("group", "seq")),
        ),
        out_specs=P(("group", "seq"), None),
        check_vma=False,
    )
```

```python
import functools
import math

import jax
import jax.numpy as jnp
from jax import lax
from jax.experimental import pallas as pl
from jax.experimental.pallas import tpu as pltpu
from jax.sharding import PartitionSpec as P


HEADS = 4
HEAD = 256
SPAN = 256
CBITS = 8
CORES = 2
F32 = jnp.float32
BF16 = jnp.bfloat16


def swap(value, bit):
    mask = 1 << bit
    return lax.ppermute(value, "seq", [(i, i ^ mask) for i in range(lax.axis_size("seq"))])


def swap_crossed(value, bit, even=0):
    size = lax.axis_size("seq")
    pairs = [
        (g * size + i, g * size + (i ^ (1 << bit) ^ ((g + even) % 2)))
        for g in range(lax.axis_size("group"))
        for i in range(size)
    ]
    return lax.ppermute(value, ("group", "seq"), pairs)


def swap_x(value):
    return lax.ppermute(value, "group", [(i, i ^ 1) for i in range(lax.axis_size("group"))])


OWN, OTHER, MINE, FAR = range(4)


def gather_rows(first, second, mine, arrived, zbits, turn):
    pieces = [(mine, 0, MINE), (arrived, 0, FAR)]
    beside = swap_crossed(first, 1)
    pieces.append((beside, 1, OWN))
    pieces.append((swap_x(beside), 1, OTHER))
    held = []
    for bit in reversed(zbits):
        flip = 1 << (bit - 1)
        got = [(swap_crossed(first, bit), flip)]
        for piece, before in held:
            got.append((swap(piece, bit), before ^ flip))
        held += got
    for at, (piece, flip) in enumerate(held):
        if flip == 1 << (zbits[0] - 1):
            side = swap_crossed(second, zbits[0], 1)
            across = swap(beside, zbits[0])
        else:
            side = swap_x(piece)
            across = swap(piece, 1)
        if at in turn:
            corner = swap_x(across)
        else:
            corner = swap(side, 1)
        pieces += [(piece, flip, OWN), (side, flip, OTHER), (across, flip ^ 1, OWN), (corner, flip ^ 1, OTHER)]
    return pieces


def first_rows(pieces, rows, device, sent_core):
    core, chip = device % CORES, device // CORES
    flips = jnp.asarray([piece[1] for piece in pieces], jnp.int32)
    halves = jnp.asarray([piece[2] for piece in pieces], jnp.int32)
    return ((chip ^ flips) * CORES + (jnp.where(halves < MINE, sent_core, core) ^ (halves & 1))) * rows


def split_kernel(parts, width, *refs):
    sources, outs = refs[:-4], refs[-4:]
    core = lax.axis_index("seq") % CORES
    sent_core = core ^ (lax.axis_index("group") % 2)
    for out, half in zip(outs, (sent_core, 1 - sent_core, core, 1 - core)):
        row = 0
        for source, offset, stride in parts:
            ref = sources[source]
            start = pl.multiple_of(offset + half * stride, width)
            out[row : row + ref.shape[0], :] = ref[:, pl.ds(start, width)]
            row += ref.shape[0]


def place_rows(dst, pieces, offset, cols, starts, base, rows):
    for at, piece in enumerate(pieces):
        start = pl.multiple_of(starts[base + at], rows)
        dst[pl.ds(start, rows), cols] = piece[offset : offset + rows, :]


def dot(a, b):
    return lax.dot_general(a, b, (((1,), (0,)), ((), ())), preferred_element_type=F32)


def dot_tt(a, b):
    return lax.dot_general(a, b, (((1,), (1,)), ((), ())), preferred_element_type=F32)


def dot_outer(a, b):
    return lax.dot_general(a, b, (((0,), (0,)), ((), ())), preferred_element_type=F32)


def keys_values_kernel(n, rows, heads, starts, xa, xb, scale, *refs):
    del scale
    pieces = refs[:n]
    ka, kb, va, vb, da, db, *sent, wk, wv = refs[n:]
    everything = slice(None)
    place_rows(wk, pieces, rows, everything, starts, 0, rows)
    place_rows(wv, pieces, 0, everything, starts, 0, rows)
    sums = [None] * heads
    for i, (x, k_out, v_out, device_sum) in enumerate(((xa, ka, va, da), (xb, kb, vb, db))):
        k = dot(x[...], wk[...]).astype(BF16)
        k_out[...] = k
        v = dot(x[...], wv[...]).astype(BF16)
        v_out[...] = v
        for h in range(heads):
            cols = slice(h * HEAD, (h + 1) * HEAD)
            state = dot_outer(k[:, cols], v[:, cols])
            device_sum[h] = state.astype(BF16)
            sums[h] = state if i == 0 else sums[h] + state
    for h in range(heads):
        sent[h][...] = sums[h].astype(BF16)


def attend_kernel(which, n, nb, rows, out_rows, heads, levels, local_bits, starts, x, k, v, other, scale, *refs):
    buckets, pieces, refs = refs[:nb], refs[nb : nb + n], refs[nb + n :]
    out, q_out, wq = refs[0], refs[1], refs[-1]
    place_rows(wq, pieces, 0, slice(None), starts, 0, rows)
    if which:
        w = refs[2]
        width = pieces[0].shape[1]
        for part in range(w.shape[1] // width):
            cols = slice(part * width, (part + 1) * width)
            place_rows(w, pieces, rows + part * out_rows, cols, starts, n, out_rows)
    row = lax.broadcasted_iota(jnp.int32, (SPAN, SPAN), 0)
    col = lax.broadcasted_iota(jnp.int32, (SPAN, SPAN), 1)
    apart = row ^ col
    causal = row >= col
    q = dot(x[...], wq[...]).astype(BF16)
    q_out[...] = q
    first = CBITS + local_bits + 1
    for h in range(heads):
        cols = slice(h * HEAD, (h + 1) * HEAD)
        states = []
        for c in range(q.shape[0] // SPAN):
            span = slice(c * SPAN, (c + 1) * SPAN)

            def weight(level):
                at = h * levels + level
                return scale[which, span, at : at + 1]

            mixing = jnp.broadcast_to(weight(0), (SPAN, SPAN))
            for level in range(1, CBITS + 1):
                mixing = jnp.where(apart >= 1 << (level - 1), weight(level), mixing)
            qh, kh, vh = q[span, cols], k[span, cols], v[span, cols]
            probs = jnp.where(causal, dot_tt(qh, kh) * mixing, 0.0).astype(BF16)
            value = dot(probs, vh)
            states.append(dot_outer(kh, vh) if c + 1 < q.shape[0] // SPAN else None)
            for b in range(1, local_bits + 1):
                half = 1 << (b - 1)
                if c & half:
                    base = (c >> b) << b
                    bucket = sum(states[base + 1 : base + half], states[base])
                    value = value + dot(qh, bucket.astype(BF16)) * weight(CBITS + b)
            for at, bucket in enumerate((other.at[h], *buckets[h::heads])):
                value = value + dot(qh, bucket[...]) * weight(first + at)
            out[span, cols] = value


def reads_kernel(which, heads, levels, level, scale, part, q, *refs):
    buckets, out = refs[:-1], refs[-1]
    for h in range(heads):
        cols = slice(h * HEAD, (h + 1) * HEAD)
        at = h * levels + level
        weight = scale[which, :, at : at + 1]
        out[:, cols] = (part[:, cols] + dot(q[:, cols], buckets[h][...]) * weight).astype(BF16)


def output_kernel(width, core_ref, mine, theirs, w_mine, w_theirs, out, block, sem):
    depth = mine.shape[1]
    core = core_ref[0]
    parts = w_mine.shape[1] // width
    low = pl.multiple_of(core * depth, depth)
    high = pl.multiple_of((1 - core) * depth, depth)
    stores = []
    for side, w in enumerate((w_mine, w_theirs)):
        for part in range(parts):
            at = side * parts + part
            cols = slice(part * width, (part + 1) * width)
            value = dot(mine[...], w[pl.ds(low, depth), cols]) + dot(theirs[...], w[pl.ds(high, depth), cols])
            block[at] = value.astype(BF16)
            half = core if side == 0 else 1 - core
            start = pl.multiple_of((half * parts + part) * width, width)
            stores.append(pltpu.make_async_copy(block.at[at], out.at[:, pl.ds(start, width)], sem.at[at]))
            stores[-1].start()
    for store in stores:
        store.wait()


ANY = pl.BlockSpec(memory_space=pl.ANY)
SMALL = pl.BlockSpec(memory_space=pltpu.SMEM)
FAST = pl.BlockSpec(memory_space=pltpu.VMEM)


def call(kernel, operands, out_specs, out_shape, scratch, flops, room=12):
    return pl.pallas_call(
        kernel,
        in_specs=[SMALL] + [FAST] * (len(operands) - 1),
        out_specs=out_specs,
        out_shape=out_shape,
        scratch_shapes=scratch,
        compiler_params=pltpu.CompilerParams(vmem_limit_bytes=room << 20),
        cost_estimate=pl.CostEstimate(flops=flops, bytes_accessed=8 << 20, transcendentals=0),
    )(*operands)


def on_device(tokens, w_qkv, w_out, level_weight):
    seq_bits = lax.axis_size("seq").bit_length() - 1
    device = lax.axis_index("seq")
    core = device % CORES
    odd_group = lax.axis_index("group") % 2
    sent_core = core ^ odd_group
    zbits = list(range(2, seq_bits))
    toks, width = tokens.shape
    levels = level_weight.shape[0]
    heads = HEADS // CORES
    cols = heads * HEAD
    head_cols = HEADS * HEAD
    local_bits = (toks // SPAN).bit_length() - 1
    rows = w_qkv.shape[0]
    out_rows, out_width = w_out.shape
    out_cols = out_width // CORES
    sd = jax.ShapeDtypeStruct

    def split(sources, parts):
        shape = (sum(sources[part[0]].shape[0] for part in parts), cols)
        first, second, mine, far = pl.pallas_call(
            functools.partial(split_kernel, parts, cols),
            out_shape=[sd(shape, BF16)] * 4,
            cost_estimate=pl.CostEstimate(flops=1 << 20, bytes_accessed=2 << 20, transcendentals=0),
        )(*sources)
        return first, second, mine, swap(far, 0)

    kv_split = split((w_qkv,), ((0, 2 * head_cols, cols), (0, head_cols, cols)))
    out_parts = out_cols // cols
    qo_split = split((w_qkv, w_out), ((0, 0, cols),) + tuple((1, n * cols, out_cols) for n in range(out_parts)))
    far_tokens = swap(tokens, 0)

    own_w = lax.dynamic_slice(level_weight, (0, core * heads, 0), (levels, heads, toks))
    far_w = swap(lax.dynamic_slice(level_weight, (0, (1 - core) * heads, 0), (levels, heads, toks)), 0)
    gains = [1.0 / math.sqrt(HEAD * max(1, 2 ** (n - 1))) for n in range(CBITS + 1)]
    gains += [1.0 / math.sqrt(SPAN * 2 ** (b - 1) * HEAD) for b in range(1, levels - CBITS)]
    first_bit = CBITS + 1 + local_bits
    shifts = jnp.asarray([max(0, n - first_bit) for n in range(levels)], jnp.int32)
    always = jnp.asarray([n < first_bit for n in range(levels)])
    block_device = jnp.stack([device, device ^ 1])
    on = jnp.where(always[None], 1, (block_device[:, None] >> shifts[None]) & 1).astype(F32)
    on = on * jnp.asarray(gains, F32)[None]
    scale = jnp.stack([own_w, far_w]) * on[:, :, None, None]
    scale = jnp.transpose(scale, (0, 3, 2, 1)).reshape(2, toks, heads * levels)

    kvp = gather_rows(*kv_split, zbits, (0,))
    qop = gather_rows(*qo_split, zbits, (0, 1))

    act = sd((toks, cols), BF16)
    state = sd((heads, HEAD, HEAD), BF16)
    ka, kb, va, vb, da, db, *totals = call(
        functools.partial(keys_values_kernel, len(kvp), rows, heads),
        [first_rows(kvp, rows, device, sent_core), tokens, far_tokens, scale, *(piece[0] for piece in kvp)],
        [FAST] * (6 + heads),
        [act] * 4 + [state] * 2 + [sd((HEAD, HEAD), BF16)] * heads,
        [pltpu.VMEM((width, cols), BF16), pltpu.VMEM((width, cols), BF16)],
        2 * 2 * toks * width * 2 * cols,
    )

    buckets = []
    for bit in range(1, seq_bits):
        for h in range(heads):
            arrived = swap(totals[h], bit)
            buckets.append(arrived)
            totals[h] = (totals[h].astype(F32) + arrived.astype(F32)).astype(BF16)

    starts = jnp.concatenate(
        [first_rows(qop, rows, device, sent_core), first_rows(qop, out_rows, device, sent_core)]
    )

    def attend(which, x, k, v, other):
        shapes = [sd((toks, cols), F32), act] + [sd((head_cols, out_cols), BF16)] * which
        return call(
            functools.partial(
                attend_kernel, which, len(qop), len(buckets) - heads, rows, out_rows, heads, levels, local_bits
            ),
            [starts, x, k, v, other, scale, *buckets[:-heads], *(piece[0] for piece in qop)],
            [FAST] * len(shapes),
            shapes,
            [pltpu.VMEM((width, cols), BF16)],
            2 * toks * width * cols,
        )

    def read(which, part, q):
        return pl.pallas_call(
            functools.partial(reads_kernel, which, heads, levels, first_bit + seq_bits - 1),
            in_specs=[FAST] * (3 + heads),
            out_specs=FAST,
            out_shape=act,
            compiler_params=pltpu.CompilerParams(vmem_limit_bytes=8 << 20),
            cost_estimate=pl.CostEstimate(flops=1 << 28, bytes_accessed=2 << 20, transcendentals=0),
        )(scale, part, q, *buckets[-heads:])

    far_part, far_q, w_mine = attend(1, far_tokens, kb, vb, da)
    w_theirs = swap(w_mine, 0)
    own_part, own_q = attend(0, tokens, ka, va, db)
    theirs = swap(read(1, far_part, far_q), 0)
    mine = read(0, own_part, own_q)
    n_blocks = CORES * out_parts
    return call(
        functools.partial(output_kernel, cols),
        [core.reshape(1).astype(jnp.int32), mine, theirs, w_mine, w_theirs],
        ANY,
        sd((toks, out_width), BF16),
        [pltpu.VMEM((n_blocks, toks, cols), BF16), pltpu.SemaphoreType.DMA((n_blocks,))],
        2 * toks * head_cols * out_width,
    )


def solution(mesh):
    return jax.shard_map(
        on_device,
        mesh=mesh,
        in_specs=(
            P(("group", "seq"), None),
            P("seq", None),
            P("seq", None),
            P(None, None, ("group", "seq")),
        ),
        out_specs=P(("group", "seq"), None),
        check_vma=False,
    )
```

```python
import functools
import math

import jax
import jax.numpy as jnp
from jax import lax
from jax.experimental import pallas as pl
from jax.experimental.pallas import tpu as pltpu
from jax.sharding import PartitionSpec as P


HEADS = 4
HEAD = 256
SPAN = 256
CBITS = 8
CORES = 2
F32 = jnp.float32
BF16 = jnp.bfloat16


def swap(value, bit):
    mask = 1 << bit
    return lax.ppermute(value, "seq", [(i, i ^ mask) for i in range(lax.axis_size("seq"))])


def swap_crossed(value, bit, even=0):
    size = lax.axis_size("seq")
    pairs = [
        (g * size + i, g * size + (i ^ (1 << bit) ^ ((g + even) % 2)))
        for g in range(lax.axis_size("group"))
        for i in range(size)
    ]
    return lax.ppermute(value, ("group", "seq"), pairs)


def swap_x(value):
    return lax.ppermute(value, "group", [(i, i ^ 1) for i in range(lax.axis_size("group"))])


OWN, OTHER, MINE, FAR = range(4)


def gather_rows(first, second, mine, arrived, chips, routes):
    made = {}

    def piece(flip, half):
        if (flip, half) not in made:
            digit = routes.get((flip, half), 0 if half else flip & -flip)
            if digit == 0:
                value = swap_x(piece(flip, 0))
            elif digit == flip:
                value = swap_crossed((first, second)[half], digit.bit_length(), half)
            else:
                value = swap(piece(flip ^ digit, half), digit.bit_length())
            made[flip, half] = value
        return made[flip, half]

    pieces = [(mine, 0, MINE), (arrived, 0, FAR)]
    for flip in range(1, chips):
        pieces += [(piece(flip, 0), flip, OWN), (piece(flip, 1), flip, OTHER)]
    return pieces


def first_rows(pieces, rows, device, sent_core):
    core, chip = device % CORES, device // CORES
    flips = jnp.asarray([piece[1] for piece in pieces], jnp.int32)
    halves = jnp.asarray([piece[2] for piece in pieces], jnp.int32)
    return ((chip ^ flips) * CORES + (jnp.where(halves < MINE, sent_core, core) ^ (halves & 1))) * rows


def split_kernel(parts, width, *refs):
    sources, outs = refs[:-4], refs[-4:]
    core = lax.axis_index("seq") % CORES
    sent_core = core ^ (lax.axis_index("group") % 2)
    for out, half in zip(outs, (sent_core, 1 - sent_core, core, 1 - core)):
        row = 0
        for source, offset, stride in parts:
            ref = sources[source]
            start = pl.multiple_of(offset + half * stride, width)
            out[row : row + ref.shape[0], :] = ref[:, pl.ds(start, width)]
            row += ref.shape[0]


def place_rows(dst, pieces, offset, cols, starts, base, rows):
    for at, piece in enumerate(pieces):
        start = pl.multiple_of(starts[base + at], rows)
        dst[pl.ds(start, rows), cols] = piece[offset : offset + rows, :]


def dot(a, b):
    return lax.dot_general(a, b, (((1,), (0,)), ((), ())), preferred_element_type=F32)


def dot_tt(a, b):
    return lax.dot_general(a, b, (((1,), (1,)), ((), ())), preferred_element_type=F32)


def dot_outer(a, b):
    return lax.dot_general(a, b, (((0,), (0,)), ((), ())), preferred_element_type=F32)


def keys_values_kernel(n, rows, heads, starts, xa, xb, scale, *refs):
    del scale
    pieces = refs[:n]
    ka, kb, va, vb, da, db, *sent, wk, wv = refs[n:]
    everything = slice(None)
    place_rows(wk, pieces, rows, everything, starts, 0, rows)
    place_rows(wv, pieces, 0, everything, starts, 0, rows)
    sums = [None] * heads
    for i, (x, k_out, v_out, device_sum) in enumerate(((xa, ka, va, da), (xb, kb, vb, db))):
        k = dot(x[...], wk[...]).astype(BF16)
        k_out[...] = k
        v = dot(x[...], wv[...]).astype(BF16)
        v_out[...] = v
        for h in range(heads):
            cols = slice(h * HEAD, (h + 1) * HEAD)
            state = dot_outer(k[:, cols], v[:, cols])
            device_sum[h] = state.astype(BF16)
            sums[h] = state if i == 0 else sums[h] + state
    for h in range(heads):
        sent[h][...] = sums[h].astype(BF16)


def attend_kernel(which, n, nb, rows, out_rows, heads, levels, local_bits, starts, x, k, v, other, scale, *refs):
    buckets, pieces, refs = refs[:nb], refs[nb : nb + n], refs[nb + n :]
    out, q_out, wq = refs[0], refs[1], refs[-1]
    place_rows(wq, pieces, 0, slice(None), starts, 0, rows)
    if which:
        w = refs[2]
        width = pieces[0].shape[1]
        for part in range(w.shape[1] // width):
            cols = slice(part * width, (part + 1) * width)
            place_rows(w, pieces, rows + part * out_rows, cols, starts, n, out_rows)
    row = lax.broadcasted_iota(jnp.int32, (SPAN, SPAN), 0)
    col = lax.broadcasted_iota(jnp.int32, (SPAN, SPAN), 1)
    apart = row ^ col
    causal = row >= col
    q = dot(x[...], wq[...]).astype(BF16)
    q_out[...] = q
    first = CBITS + local_bits + 1
    for h in range(heads):
        cols = slice(h * HEAD, (h + 1) * HEAD)
        states = []
        for c in range(q.shape[0] // SPAN):
            span = slice(c * SPAN, (c + 1) * SPAN)

            def weight(level):
                at = h * levels + level
                return scale[which, span, at : at + 1]

            mixing = jnp.broadcast_to(weight(0), (SPAN, SPAN))
            for level in range(1, CBITS + 1):
                mixing = jnp.where(apart >= 1 << (level - 1), weight(level), mixing)
            qh, kh, vh = q[span, cols], k[span, cols], v[span, cols]
            probs = jnp.where(causal, dot_tt(qh, kh) * mixing, 0.0).astype(BF16)
            value = dot(probs, vh)
            states.append(dot_outer(kh, vh) if c + 1 < q.shape[0] // SPAN else None)
            for b in range(1, local_bits + 1):
                half = 1 << (b - 1)
                if c & half:
                    base = (c >> b) << b
                    bucket = sum(states[base + 1 : base + half], states[base])
                    value = value + dot(qh, bucket.astype(BF16)) * weight(CBITS + b)
            for at, bucket in enumerate((other.at[h], *buckets[h::heads])):
                value = value + dot(qh, bucket[...]) * weight(first + at)
            out[span, cols] = value


def reads_kernel(which, heads, levels, level, scale, part, q, *refs):
    buckets, out = refs[:-1], refs[-1]
    for h in range(heads):
        cols = slice(h * HEAD, (h + 1) * HEAD)
        at = h * levels + level
        weight = scale[which, :, at : at + 1]
        out[:, cols] = (part[:, cols] + dot(q[:, cols], buckets[h][...]) * weight).astype(BF16)


def output_kernel(width, core_ref, mine, theirs, w_mine, w_theirs, out, block, sem):
    depth = mine.shape[1]
    core = core_ref[0]
    parts = w_mine.shape[1] // width
    low = pl.multiple_of(core * depth, depth)
    high = pl.multiple_of((1 - core) * depth, depth)
    stores = []
    for side, w in enumerate((w_mine, w_theirs)):
        for part in range(parts):
            at = side * parts + part
            cols = slice(part * width, (part + 1) * width)
            value = dot(mine[...], w[pl.ds(low, depth), cols]) + dot(theirs[...], w[pl.ds(high, depth), cols])
            block[at] = value.astype(BF16)
            half = core if side == 0 else 1 - core
            start = pl.multiple_of((half * parts + part) * width, width)
            stores.append(pltpu.make_async_copy(block.at[at], out.at[:, pl.ds(start, width)], sem.at[at]))
            stores[-1].start()
    for store in stores:
        store.wait()


ANY = pl.BlockSpec(memory_space=pl.ANY)
SMALL = pl.BlockSpec(memory_space=pltpu.SMEM)
FAST = pl.BlockSpec(memory_space=pltpu.VMEM)


def call(kernel, operands, out_specs, out_shape, scratch, flops, room=12):
    return pl.pallas_call(
        kernel,
        in_specs=[SMALL] + [FAST] * (len(operands) - 1),
        out_specs=out_specs,
        out_shape=out_shape,
        scratch_shapes=scratch,
        compiler_params=pltpu.CompilerParams(vmem_limit_bytes=room << 20),
        cost_estimate=pl.CostEstimate(flops=flops, bytes_accessed=8 << 20, transcendentals=0),
    )(*operands)


def on_device(tokens, w_qkv, w_out, level_weight):
    seq_bits = lax.axis_size("seq").bit_length() - 1
    device = lax.axis_index("seq")
    core = device % CORES
    odd_group = lax.axis_index("group") % 2
    sent_core = core ^ odd_group
    toks, width = tokens.shape
    levels = level_weight.shape[0]
    heads = HEADS // CORES
    cols = heads * HEAD
    head_cols = HEADS * HEAD
    local_bits = (toks // SPAN).bit_length() - 1
    rows = w_qkv.shape[0]
    out_rows, out_width = w_out.shape
    out_cols = out_width // CORES
    sd = jax.ShapeDtypeStruct

    def split(sources, parts):
        shape = (sum(sources[part[0]].shape[0] for part in parts), cols)
        first, second, mine, far = pl.pallas_call(
            functools.partial(split_kernel, parts, cols),
            out_shape=[sd(shape, BF16)] * 4,
            cost_estimate=pl.CostEstimate(flops=1 << 20, bytes_accessed=2 << 20, transcendentals=0),
        )(*sources)
        return first, second, mine, swap(far, 0)

    kv_split = split((w_qkv,), ((0, 2 * head_cols, cols), (0, head_cols, cols)))
    out_parts = out_cols // cols
    qo_split = split((w_qkv, w_out), ((0, 0, cols),) + tuple((1, n * cols, out_cols) for n in range(out_parts)))
    far_tokens = swap(tokens, 0)

    own_w = lax.dynamic_slice(level_weight, (0, core * heads, 0), (levels, heads, toks))
    far_w = swap(lax.dynamic_slice(level_weight, (0, (1 - core) * heads, 0), (levels, heads, toks)), 0)
    gains = [1.0 / math.sqrt(HEAD * max(1, 2 ** (n - 1))) for n in range(CBITS + 1)]
    gains += [1.0 / math.sqrt(SPAN * 2 ** (b - 1) * HEAD) for b in range(1, levels - CBITS)]
    first_bit = CBITS + 1 + local_bits
    shifts = jnp.asarray([max(0, n - first_bit) for n in range(levels)], jnp.int32)
    always = jnp.asarray([n < first_bit for n in range(levels)])
    block_device = jnp.stack([device, device ^ 1])
    on = jnp.where(always[None], 1, (block_device[:, None] >> shifts[None]) & 1).astype(F32)
    on = on * jnp.asarray(gains, F32)[None]
    scale = jnp.stack([own_w, far_w]) * on[:, :, None, None]
    scale = jnp.transpose(scale, (0, 3, 2, 1)).reshape(2, toks, heads * levels)

    chips = lax.axis_size("seq") // CORES
    kvp = gather_rows(*kv_split, chips, KV_ROUTES)
    qop = gather_rows(*qo_split, chips, QO_ROUTES)

    act = sd((toks, cols), BF16)
    state = sd((heads, HEAD, HEAD), BF16)
    ka, kb, va, vb, da, db, *totals = call(
        functools.partial(keys_values_kernel, len(kvp), rows, heads),
        [first_rows(kvp, rows, device, sent_core), tokens, far_tokens, scale, *(piece[0] for piece in kvp)],
        [FAST] * (6 + heads),
        [act] * 4 + [state] * 2 + [sd((HEAD, HEAD), BF16)] * heads,
        [pltpu.VMEM((width, cols), BF16), pltpu.VMEM((width, cols), BF16)],
        2 * 2 * toks * width * 2 * cols,
    )

    buckets = []
    for bit in range(1, seq_bits):
        for h in range(heads):
            arrived = swap(totals[h], bit)
            buckets.append(arrived)
            totals[h] = (totals[h].astype(F32) + arrived.astype(F32)).astype(BF16)

    starts = jnp.concatenate(
        [first_rows(qop, rows, device, sent_core), first_rows(qop, out_rows, device, sent_core)]
    )

    def attend(which, x, k, v, other):
        shapes = [sd((toks, cols), F32), act] + [sd((head_cols, out_cols), BF16)] * which
        return call(
            functools.partial(
                attend_kernel, which, len(qop), len(buckets) - heads, rows, out_rows, heads, levels, local_bits
            ),
            [starts, x, k, v, other, scale, *buckets[:-heads], *(piece[0] for piece in qop)],
            [FAST] * len(shapes),
            shapes,
            [pltpu.VMEM((width, cols), BF16)],
            2 * toks * width * cols,
        )

    def read(which, part, q):
        return pl.pallas_call(
            functools.partial(reads_kernel, which, heads, levels, first_bit + seq_bits - 1),
            in_specs=[FAST] * (3 + heads),
            out_specs=FAST,
            out_shape=act,
            compiler_params=pltpu.CompilerParams(vmem_limit_bytes=8 << 20),
            cost_estimate=pl.CostEstimate(flops=1 << 28, bytes_accessed=2 << 20, transcendentals=0),
        )(scale, part, q, *buckets[-heads:])

    far_part, far_q, w_mine = attend(1, far_tokens, kb, vb, da)
    w_theirs = swap(w_mine, 0)
    own_part, own_q = attend(0, tokens, ka, va, db)
    theirs = swap(read(1, far_part, far_q), 0)
    mine = read(0, own_part, own_q)
    n_blocks = CORES * out_parts
    return call(
        functools.partial(output_kernel, cols),
        [core.reshape(1).astype(jnp.int32), mine, theirs, w_mine, w_theirs],
        ANY,
        sd((toks, out_width), BF16),
        [pltpu.VMEM((n_blocks, toks, cols), BF16), pltpu.SemaphoreType.DMA((n_blocks,))],
        2 * toks * head_cols * out_width,
    )


KV_ROUTES = {(1, 1): 1, (3, 0): 2, (3, 1): 1, (5, 1): 1}
QO_ROUTES = {(2, 1): 2, (3, 0): 2, (5, 1): 1}


def solution(mesh):
    return jax.shard_map(
        on_device,
        mesh=mesh,
        in_specs=(
            P(("group", "seq"), None),
            P("seq", None),
            P("seq", None),
            P(None, None, ("group", "seq")),
        ),
        out_specs=P(("group", "seq"), None),
        check_vma=False,
    )
```
